32 devices in a mesh: ctx: 16 (over z, y, x), head: 2 (over core).
Axes of the slice: x: 2, y: 2, z: 4, core: 2. Of those that a mesh axis runs over, the one named last changes fastest.
Arguments:
- q_heads: bfloat16 [32, 24576], P('ctx', 'head'), may hold values from -6 to 6
- w_uk: bfloat16 [128, 128, 512], P('head'), may hold values from -1 to 1
- latent_t: bfloat16 [576, 16384], P(None, 'ctx'), may hold values from -48 to 48
- index_query: bfloat16 [32, 8192], P('ctx', 'head'), may hold values from -48 to 48
- index_key: bfloat16 [16384, 128], P('ctx'), may hold values from -4 to 4
- head_weight: bfloat16 [32, 64], P('ctx', 'head'), may hold values from 0.099609375 to 1
- query_pos: int32 [32], replicated, may hold values from 8192 to 16383
- key_start: int32 [32], replicated, may hold values from 0 to 4095
Outputs:
- grad_index_query: float32 [32, 8192], P('ctx', 'head')
- grad_index_key: float32 [16384, 128], P('ctx')
- grad_head_weight: float32 [32, 64], P('ctx', 'head')
The draws below stay inside these ranges and needn't reach their ends.
All inputs are finite; a program needn't handle non-finite values.
Results may differ from the reference program's by a relative error of at most 0.0035.
Values may be sent and summed in bfloat16 or wider, within the bound.
No kernel may reach another device: no remote copies, remote signals or barrier semaphores. Data moves between devices by JAX's collectives and lax.ppermute only.
A program may use at most 192 MiB of HBM per device.

```python
import math
import jax
import jax.numpy as jnp
from jax import lax

MLA_HEADS = 128
LATENT_RANK = 512
ROPE_DIM = 64
NOPE_DIM = 128
INDEX_HEADS = 64
INDEX_DIM = 128
ALL_KEYS = 16384
QUERIES = 32


def attention_parts(key):
    base = jax.random.fold_in(key, 17)
    key_query, key_weight, key_latent = jax.random.split(base, 3)
    width = NOPE_DIM + ROPE_DIM
    queries = jnp.clip(jax.random.normal(key_query, (QUERIES, MLA_HEADS * width), jnp.float32), -6.0, 6.0)
    absorb_weight = jnp.clip(jax.random.normal(key_weight, (MLA_HEADS, NOPE_DIM, LATENT_RANK), jnp.float32) * NOPE_DIM ** (-0.5), -1.0, 1.0)
    latent_all = jnp.clip(jax.random.normal(key_latent, (LATENT_RANK + ROPE_DIM, ALL_KEYS), jnp.float32), -4.0, 4.0)
    return (queries, absorb_weight, latent_all)


def index_parts(key):
    base = jax.random.fold_in(key, 29)
    key_query, key_keys = jax.random.split(base, 2)
    queries = jnp.clip(jax.random.normal(key_query, (QUERIES, INDEX_HEADS * INDEX_DIM), jnp.float32), -6.0, 6.0)
    keys_all = jnp.clip(jax.random.normal(key_keys, (ALL_KEYS, INDEX_DIM), jnp.float32), -4.0, 4.0)
    return (queries, keys_all)


def draw_q_heads(key, part):
    return attention_parts(key)[0].astype(jnp.bfloat16)


def draw_w_uk(key, part):
    return attention_parts(key)[1].astype(jnp.bfloat16)


def draw_latent_t(key, part):
    return attention_parts(key)[2].astype(jnp.bfloat16)


def draw_index_query(key, part):
    return index_parts(key)[0].astype(jnp.bfloat16)


def draw_index_key(key, part):
    return index_parts(key)[1].astype(jnp.bfloat16)


def place_ends(values, key, least, top_value):
    spot = [jax.random.randint(jax.random.fold_in(key, axis), (), 0, length) for axis, length in enumerate(values.shape)]
    main_axis = values.shape.index(max(values.shape))
    next_to = spot[:main_axis] + [(spot[main_axis] + 1) % values.shape[main_axis]] + spot[main_axis + 1:]
    return values.at[tuple(spot)].set(least).at[tuple(next_to)].set(top_value)


def levels(key, dims, cuts, least, high):
    def one(dim, blocks):
        heights = jax.random.uniform(jax.random.fold_in(jax.random.fold_in(key, 6), dim), (blocks,), jnp.float32, least / len(cuts), high / len(cuts))
        return jnp.repeat(jnp.exp(heights), dims[dim] // blocks).reshape((-1,) + (1,) * (len(dims) - dim - 1))

    gain = one(*cuts[0])
    for cut in cuts[1:]:
        gain = gain * one(*cut)
    return gain


def setup_inputs(seed: int = 0) -> dict:
    keys = jax.random.split(jax.random.key(seed), 9)
    return {
        "q_heads": draw_q_heads(jax.random.fold_in(keys[8], 71), 0),
        "w_uk": draw_w_uk(jax.random.fold_in(keys[8], 71), 0),
        "latent_t": draw_latent_t(jax.random.fold_in(keys[8], 71), 0),
        "index_query": draw_index_query(jax.random.fold_in(keys[8], 71), 0),
        "index_key": draw_index_key(jax.random.fold_in(keys[8], 71), 0),
        "head_weight": jnp.clip(jnp.exp(math.log(1.0) - 2.306499 * jax.random.uniform(keys[5], (QUERIES, INDEX_HEADS), jnp.float32) ** levels(keys[5], (QUERIES, INDEX_HEADS), ((0, 16), (1, 2)), -0.2, 0.2)), 0.099609375, 1.0).astype(jnp.bfloat16),
        "query_pos": place_ends(jax.random.randint(keys[6], (QUERIES,), ALL_KEYS // 2, ALL_KEYS), jax.random.fold_in(keys[6], 1), ALL_KEYS // 2, ALL_KEYS - 1).astype(jnp.int32),
        "key_start": place_ends(jax.random.randint(keys[7], (QUERIES,), 0, ALL_KEYS // 4), jax.random.fold_in(keys[7], 1), 0, (ALL_KEYS // 4) - 1).astype(jnp.int32),
    }


masked_score = -1.0e30


def reference(q_heads, w_uk, latent_t, index_query, index_key, head_weight, query_pos, key_start):
    width = NOPE_DIM + ROPE_DIM
    shaped = q_heads.reshape(QUERIES, MLA_HEADS, width)
    folded = jnp.einsum('qhn,hnc->qhc', shaped[:, :, :NOPE_DIM].astype(jnp.float32), w_uk.astype(jnp.float32))
    latent_query = jnp.concatenate([folded.astype(jnp.bfloat16), shaped[:, :, NOPE_DIM:]], axis=2)
    index_blocks = index_query.reshape(QUERIES, INDEX_HEADS, INDEX_DIM)
    index_scale = (INDEX_DIM * INDEX_HEADS) ** -0.5
    score_scale = width ** -0.5
    scaled_weights = head_weight.astype(jnp.float32) * index_scale
    key_ids = jnp.arange(ALL_KEYS, dtype=jnp.int32)

    def one_query(grad_key, row_items):
        latent_row, index_row, weight_row, position, first_key = row_items
        visible = (key_ids >= first_key) & (key_ids <= position)
        raw_scores = jnp.dot(latent_row, latent_t, preferred_element_type=jnp.float32) * score_scale
        scores = jnp.where(visible[None, :], raw_scores, masked_score)
        row_peak = jnp.max(scores, axis=1, keepdims=True)
        powers = jnp.exp(scores - row_peak)
        row_total = jnp.sum(powers, axis=1, keepdims=True)
        target = jnp.sum(powers / row_total, axis=0) / MLA_HEADS
        dotted = jnp.dot(index_row, index_key.T, preferred_element_type=jnp.float32)
        active = jnp.maximum(dotted, 0.0)
        index_total = jnp.sum(active * weight_row[:, None], axis=0)
        index_masked = jnp.where(visible, index_total, masked_score)
        index_peak = jnp.max(index_masked)
        index_powers = jnp.exp(index_masked - index_peak)
        predicted = index_powers / jnp.sum(index_powers)
        misfit = (predicted - target) * ALL_KEYS
        slopes = jnp.where(dotted > 0, misfit[None, :] * weight_row[:, None], 0.0).astype(jnp.bfloat16)
        grad_query = jnp.dot(slopes, index_key, preferred_element_type=jnp.float32)
        grad_weight = jnp.sum(misfit[None, :] * active, axis=1) * index_scale
        grad_key = grad_key + jnp.dot(slopes.T, index_row, preferred_element_type=jnp.float32)
        return grad_key, (grad_query.reshape(-1), grad_weight)

    start_grad = jnp.zeros((ALL_KEYS, INDEX_DIM), jnp.float32)
    grad_key, outputs = lax.scan(one_query, start_grad, (latent_query, index_blocks, scaled_weights, query_pos, key_start))
    return outputs[0], grad_key, outputs[1]
```

```python
import numpy as np
import jax
import jax.numpy as jnp
from jax import lax
from jax.sharding import PartitionSpec as P

MLA_HEADS = 128
ROPE_DIM = 64
NOPE_DIM = 128
INDEX_HEADS = 64
INDEX_DIM = 128


masked_score = -1e30


def exchange_stages(size):
    bits = size.bit_length() - 1
    stages = []
    while bits > 0:
        take = 2 if bits >= 2 else 1
        bits -= take
        stages.append([k << bits for k in range(1 << take)])
    return stages


def gather_relative(block, axis, size):
    offsets = [0]
    for masks in exchange_stages(size):
        parts = [block]
        for mask in masks[1:]:
            parts.append(lax.ppermute(block, axis, [(i, i ^ mask) for i in range(size)]))
        block = jnp.concatenate(parts, axis=0)
        offsets = [mask ^ offset for mask in masks for offset in offsets]
    return block, np.array(offsets)


def pair_sum(part, axis):
    return part + lax.ppermute(part, axis, [(0, 1), (1, 0)])


def shards(q_heads, w_uk, latent_t, index_query, index_key, head_weight, query_pos, key_start):
    own_rows = q_heads.shape[0]
    ctx = lax.axis_size("ctx")
    me = lax.axis_index("ctx")
    key_count = latent_t.shape[1]
    local_heads = w_uk.shape[0]
    index_local = head_weight.shape[1]
    width = NOPE_DIM + ROPE_DIM
    score_scale = width ** (-0.5)
    index_scale = (INDEX_DIM * INDEX_HEADS) ** (-0.5)

    pad = jnp.zeros((own_rows, -index_local % 128), head_weight.dtype)
    packed = jnp.concatenate([q_heads, index_query, head_weight, pad], axis=1)
    gathered, offsets = gather_relative(packed, "ctx", ctx)
    queries = gathered.shape[0]
    q_cols, i_cols = q_heads.shape[1], index_query.shape[1]
    shaped = gathered[:, :q_cols].reshape(queries, local_heads, width)
    index_blocks = gathered[:, q_cols : q_cols + i_cols].reshape(queries, index_local, INDEX_DIM)
    weight_all = gathered[:, q_cols + i_cols : q_cols + i_cols + index_local]

    rows = ((me ^ offsets)[:, None] * own_rows + np.arange(own_rows)[None, :]).reshape(-1)
    first, last = key_start[rows], query_pos[rows]
    key_ids = me * key_count + jnp.arange(key_count, dtype=jnp.int32)
    visible = (key_ids[None, :] >= first[:, None]) & (key_ids[None, :] <= last[:, None])

    scaled_weights = weight_all.astype(jnp.float32) * index_scale
    dotted = jnp.einsum("qjd,kd->qjk", index_blocks, index_key, preferred_element_type=jnp.float32)
    active = jnp.maximum(dotted, 0.0)
    index_total = pair_sum(jnp.sum(active * scaled_weights[:, :, None], axis=1), "head")
    index_masked = jnp.where(visible, index_total, masked_score)
    index_peak = jnp.max(index_masked, axis=1)
    index_powers = jnp.exp(index_masked - index_peak[:, None])
    index_lse = index_peak + jnp.log(jnp.sum(index_powers, axis=1))

    folded = jnp.einsum("rhn,hnc->rhc", shaped[:, :, :NOPE_DIM], w_uk, preferred_element_type=jnp.float32)
    latent_query = jnp.concatenate([folded.astype(jnp.bfloat16), shaped[:, :, NOPE_DIM:]], axis=2)
    raw_scores = jnp.einsum("rhc,ck->rhk", latent_query, latent_t, preferred_element_type=jnp.float32)
    scores = jnp.where(visible[:, None, :], raw_scores * score_scale, masked_score)
    peak = jnp.max(scores, axis=2)
    powers = jnp.exp(scores - peak[:, :, None])
    lse = peak + jnp.log(jnp.sum(powers, axis=2))

    stats = jnp.concatenate([lse, jnp.broadcast_to(index_lse[:, None], (queries, -local_heads % 128))], axis=1)
    order = np.empty(ctx, np.int32)
    order[offsets] = np.arange(ctx)
    back = jnp.asarray(order)[me ^ np.arange(ctx)]
    stats_abs = stats.reshape(ctx, own_rows, -1)[back].reshape(stats.shape)
    sent = jnp.broadcast_to(stats_abs[None], (ctx, *stats.shape))
    every = lax.all_to_all(sent, "ctx", 0, 0, tiled=True)
    top = jnp.max(every, axis=0)
    whole = top + jnp.log(jnp.sum(jnp.exp(every - top[None]), axis=0))
    whole = whole.reshape(ctx, own_rows, -1)[me ^ offsets].reshape(stats.shape)
    factor = jnp.exp(lse - whole[:, :local_heads]) * jnp.exp(peak - lse)
    index_factor = jnp.exp(index_peak - whole[:, local_heads])

    target = pair_sum(jnp.sum(powers * factor[:, :, None], axis=1), "head") / MLA_HEADS
    predicted = index_powers * index_factor[:, None]
    misfit = (predicted - target) * (key_count * ctx)
    slopes = jnp.where(dotted > 0, misfit[:, None, :] * scaled_weights[:, :, None], 0.0).astype(jnp.bfloat16)
    grad_query_part = jnp.einsum("qjk,kd->qjd", slopes, index_key, preferred_element_type=jnp.float32)
    to_owner = grad_query_part.reshape(ctx, own_rows, i_cols)[back]
    grad_query = jnp.sum(lax.all_to_all(to_owner, "ctx", 0, 0, tiled=True), axis=0)
    grad_key_part = jnp.einsum("qjk,qjd->kd", slopes, index_blocks, preferred_element_type=jnp.float32)
    grad_key = pair_sum(grad_key_part, "head")
    along = (grad_query * index_query.astype(jnp.float32)).reshape(own_rows, index_local, INDEX_DIM)
    grad_weight = jnp.sum(along, axis=2) / head_weight.astype(jnp.float32)
    return grad_query, grad_key, grad_weight


def solution(mesh):
    placed = (
        P("ctx", "head"),
        P("head", None, None),
        P(None, "ctx"),
        P("ctx", "head"),
        P("ctx", None),
        P("ctx", "head"),
        P(),
        P(),
    )
    return jax.shard_map(
        shards,
        mesh=mesh,
        in_specs=placed,
        out_specs=(P("ctx", "head"), P("ctx", None), P("ctx", "head")),
        check_vma=False,
    )
```

```python
import functools
import math

import jax
import jax.numpy as jnp
from jax import lax
from jax.experimental import pallas as pl
from jax.experimental.pallas import tpu as pltpu
from jax.sharding import PartitionSpec as P


MLA_HEADS = 128
ROPE_DIM = 64
NOPE_DIM = 128
INDEX_HEADS = 64
INDEX_DIM = 128
WIDTH = NOPE_DIM + ROPE_DIM
LANES = 128


MASKED = -1e30
HEADS_A_STEP = 8
LOG2E = math.log2(math.e)
f32 = jnp.float32
bf16 = jnp.bfloat16
HBM_WHOLE = pl.BlockSpec(memory_space=pltpu.HBM)
VMEM_WHOLE = pl.BlockSpec(memory_space=pltpu.VMEM)
SMEM_WHOLE = pl.BlockSpec(memory_space=pltpu.SMEM)


def exchange_stages(size):
    bits = size.bit_length() - 1
    stages = []
    while bits > 0:
        take = 2 if bits >= 2 else 1
        bits -= take
        stages.append([k << bits for k in range(1 << take)])
    return stages


def send(block, axis, size, mask):
    return lax.ppermute(block, axis, [(i, i ^ mask) for i in range(size)])


def gather_pieces(own, axis, size):
    *stages, last = exchange_stages(size)
    early = [send(own, axis, size, mask) for mask in last[1:]]
    blocks, offsets = own, [0]
    for masks in stages:
        parts = [blocks] + [send(blocks, axis, size, mask) for mask in masks[1:]]
        blocks = jnp.concatenate(parts[(len(offsets) == 1) :], axis=0)
        if len(offsets) == 1:
            blocks = blocks if len(stages) == 1 else jnp.concatenate([own, blocks], axis=0)
        offsets = [mask ^ offset for mask in masks for offset in offsets]
    if not stages:
        return [own, *early], list(last)
    rest = blocks if len(stages) == 1 else blocks[1:]
    late = [send(rest, axis, size, mask) for mask in last[1:]]
    pieces, order = [own, rest], list(offsets)
    for mask, own_piece, rest_piece in zip(last[1:], early, late, strict=True):
        pieces += [own_piece, rest_piece]
        order += [mask ^ offset for offset in offsets]
    return pieces, order


def pair_swap(part):
    return lax.ppermute(part, "head", [(0, 1), (1, 0)])


def params(held=0):
    return pltpu.CompilerParams(vmem_limit_bytes=(16 << 20) if held <= (16 << 20) else (60 << 20))


def row_column(shape, values):
    row = lax.broadcasted_iota(jnp.int32, shape, 0)
    out = jnp.zeros(shape, jnp.int32)
    for i, value in enumerate(values):
        out = jnp.where(row == i, value, out)
    return out


def bias_kernel(offsets, own_rows, keys, pos_ref, start_ref, bias_ref):
    queries = bias_ref.shape[0]
    me = lax.axis_index("ctx")
    places = [(me ^ int(off)) * own_rows + r for off in offsets for r in range(own_rows)]
    ids = me * keys + lax.broadcasted_iota(jnp.int32, (queries, keys), 1)
    first = row_column((queries, LANES), [start_ref[p] for p in places])[:, :1]
    last = row_column((queries, LANES), [pos_ref[p] for p in places])[:, :1]
    bias_ref[...] = jnp.where((ids >= first) & (ids <= last), 0.0, MASKED)


def fetch_kernel(*refs):
    count = (len(refs) - 1) // 2
    copies = [pltpu.make_async_copy(refs[i], refs[count + i], refs[-1].at[i]) for i in range(count)]
    for copy in copies:
        copy.start()
    for copy in copies:
        copy.wait()


def index_kernel(own_rows, heads, query_cols, key_ref, *refs):
    *piece_refs, rows_ref, gate_ref, part_ref, stack_ref = refs
    queries = rows_ref.shape[0]
    keys = key_ref.shape[0]
    at = 0
    for piece in piece_refs:
        for i in range(piece.shape[0]):
            rows_ref[at : at + own_rows, :] = piece[i]
            at += own_rows
    scale = (INDEX_DIM * INDEX_HEADS) ** (-0.5)
    weights = rows_ref[:, query_cols + heads * INDEX_DIM :].astype(f32) * scale
    for j in range(heads):
        col = query_cols + j * INDEX_DIM
        stack_ref[j * queries : (j + 1) * queries, :] = rows_ref[:, col : col + INDEX_DIM]
    chunk = 8
    total = jnp.zeros((queries, keys), f32)
    for c in range(0, heads, chunk):
        left = stack_ref[c * queries : (c + chunk) * queries, :]
        dotted = lax.dot_general(left, key_ref[...], (((1,), (1,)), ((), ())), preferred_element_type=f32)
        for j in range(chunk):
            one = dotted[j * queries : (j + 1) * queries]
            gate = jnp.where(one > 0, weights[:, c + j : c + j + 1], 0.0)
            gate_ref[c + j] = gate
            total = total + gate * one
    part_ref[...] = total


def score_kernel(rows_ref, w_ref, latent_ref, bias_ref, power_ref, peak_ref, lse_ref, *left_refs):
    queries = bias_ref.shape[0]
    heads, _, rank = w_ref.shape
    chunk = HEADS_A_STEP
    scale = WIDTH ** (-0.5)
    lane = lax.broadcasted_iota(jnp.int32, (queries, LANES), 1)

    def absorb(c, left_ref):
        for i in range(chunk):
            h = c * chunk + i
            own = rows_ref[:, h * WIDTH : (h + 1) * WIDTH]
            folded = jnp.dot(own[:, :NOPE_DIM], w_ref[h], preferred_element_type=f32)
            left_ref[i * queries : (i + 1) * queries, :rank] = folded.astype(bf16)
            left_ref[i * queries : (i + 1) * queries, rank:] = own[:, NOPE_DIM:]

    peaks = jnp.zeros((queries, LANES), f32)
    lses = jnp.zeros((queries, LANES), f32)
    absorb(0, left_refs[0])
    for c in range(heads // chunk):
        raw = jnp.dot(left_refs[c % len(left_refs)][...], latent_ref[...], preferred_element_type=f32)
        if c + 1 < heads // chunk:
            absorb(c + 1, left_refs[(c + 1) % len(left_refs)])
        for i in range(chunk):
            h = c * chunk + i
            one = raw[i * queries : (i + 1) * queries] + bias_ref[...]
            top = jnp.max(one, axis=1, keepdims=True)
            power = jnp.exp2((one - top) * (scale * LOG2E))
            power_ref[h] = power
            total = jnp.sum(power, axis=1, keepdims=True)
            peak = top * scale
            peaks = jnp.where(lane == h, peak, peaks)
            lses = jnp.where(lane == h, peak + jnp.log(total), lses)
    peak_ref[...] = peaks
    lse_ref[...] = lses


def packed_rows(heads, queries):
    a_row = LANES // heads
    return a_row, queries // a_row


def stats_kernel(offsets, own_rows, heads, part_ref, other_ref, bias_ref, lse_ref, send_ref, power_ref, peak_ref):
    queries = part_ref.shape[0]
    me = lax.axis_index("ctx")
    score = (part_ref[...] + other_ref[...]) + bias_ref[...]
    peak = jnp.max(score, axis=1, keepdims=True)
    power = jnp.exp(score - peak)
    power_ref[...] = power
    lse = peak + jnp.log(jnp.sum(power, axis=1, keepdims=True))
    lane = lax.broadcasted_iota(jnp.int32, (queries, LANES), 1)
    row = lax.broadcasted_iota(jnp.int32, (queries, LANES), 0)
    stats = jnp.where(lane == heads, lse, lse_ref[...])
    peak_ref[...] = jnp.broadcast_to(peak, (queries, LANES))
    place = {int(off): b for b, off in enumerate(offsets)}
    a_row, count = packed_rows(heads, queries)
    for away in range(len(offsets)):
        order = [place[away ^ int(off)] for off in offsets]
        moved = jnp.concatenate([stats[b * own_rows : (b + 1) * own_rows] for b in order], axis=0)
        packed = moved[:count]
        for i in range(1, a_row):
            packed = jnp.where(lane[:count] < i * heads, packed, pltpu.roll(moved[i * count : (i + 1) * count], i * heads, 1))
        line = jnp.sum(jnp.where(lane == row, moved[:, heads : heads + 1], 0.0), axis=0, keepdims=True)
        for i in range(count):
            send_ref[me ^ away, :, i * LANES : (i + 1) * LANES] = packed[i : i + 1]
        send_ref[me ^ away, :, count * LANES :] = line


def target_kernel(heads, every_ref, peak_ref, index_peak_ref, power_ref, index_power_ref, target_ref, predicted_ref):
    queries = peak_ref.shape[0]
    a_row, count = packed_rows(heads, queries)
    lines = []
    for i in range(count + 1):
        part = every_ref[:, 0, i * LANES : (i + 1) * LANES]
        top = jnp.max(part, axis=0, keepdims=True)
        lines.append(top + jnp.log(jnp.sum(jnp.exp(part - top), axis=0, keepdims=True)))
    packed = jnp.concatenate(lines[:count], axis=0)
    whole = jnp.concatenate([packed] + [pltpu.roll(packed, LANES - i * heads, 1) for i in range(1, a_row)], axis=0)
    lane = lax.broadcasted_iota(jnp.int32, (queries, LANES), 1)
    row = lax.broadcasted_iota(jnp.int32, (queries, LANES), 0)
    index_whole = jnp.sum(jnp.where(lane == row, lines[count], 0.0), axis=1, keepdims=True)
    factor = jnp.exp(peak_ref[...] - whole)
    predicted_ref[...] = index_power_ref[...] * jnp.exp(index_peak_ref[:, :1] - index_whole)
    total = power_ref[0] * factor[:, :1]
    for h in range(1, heads):
        total = total + power_ref[h] * factor[:, h : h + 1]
    target_ref[...] = total


def slope_kernel(offsets, own_rows, all_keys, predicted_ref, target_ref, other_ref, gate_ref, key_ref, slope_ref, send_ref):
    heads, queries, _ = gate_ref.shape
    me = lax.axis_index("ctx")
    target = (target_ref[...] + other_ref[...]) / MLA_HEADS
    misfit = (predicted_ref[...] - target) * all_keys
    chunk = 8
    for c in range(0, heads, chunk):
        slopes = jnp.concatenate([(misfit * gate_ref[c + j]).astype(bf16) for j in range(chunk)], axis=0)
        slope_ref[c * queries : (c + chunk) * queries, :] = slopes
        grad = jnp.dot(slopes, key_ref[...], preferred_element_type=f32).astype(send_ref.dtype)
        for j in range(chunk):
            col = (c + j) * INDEX_DIM
            for b, off in enumerate(offsets):
                at = j * queries + b * own_rows
                send_ref[me ^ int(off), :, col : col + INDEX_DIM] = grad[at : at + own_rows]


def shards(q_heads, w_uk, latent_t, index_query, index_key, head_weight, query_pos, key_start):
    own_rows = q_heads.shape[0]
    ctx = lax.axis_size("ctx")
    latent_dim, keys = latent_t.shape
    local_heads, _, _ = w_uk.shape
    index_local = head_weight.shape[1]
    queries = own_rows * ctx
    shape = jax.ShapeDtypeStruct

    pad = jnp.zeros((own_rows, -index_local % LANES), bf16)
    own = jnp.concatenate([q_heads, index_query, head_weight, pad], axis=1)
    pieces, offsets = gather_pieces(own[None], "ctx", ctx)

    bias = pl.pallas_call(
        functools.partial(bias_kernel, offsets, own_rows, keys),
        out_shape=shape((queries, keys), f32),
        in_specs=[SMEM_WHOLE] * 2,
        out_specs=VMEM_WHOLE,
        compiler_params=params(),
        name="bias",
    )(query_pos, key_start)
    held = (w_uk, latent_t, index_key)
    w_uk, latent_t, index_key = pl.pallas_call(
        fetch_kernel,
        out_shape=tuple(shape(a.shape, a.dtype) for a in held),
        in_specs=[HBM_WHOLE] * len(held),
        out_specs=(VMEM_WHOLE,) * len(held),
        scratch_shapes=[pltpu.SemaphoreType.DMA((len(held),))],
        compiler_params=params(),
        name="fetch",
    )(*held)

    rows, gate, part, stack = pl.pallas_call(
        functools.partial(index_kernel, own_rows, index_local, q_heads.shape[1]),
        out_shape=(
            shape((queries, own.shape[1]), bf16),
            shape((index_local, queries, keys), f32),
            shape((queries, keys), f32),
            shape((index_local * queries, INDEX_DIM), bf16),
        ),
        in_specs=[VMEM_WHOLE] * (1 + len(pieces)),
        out_specs=(VMEM_WHOLE,) * 4,
        compiler_params=params(4 * index_local * queries * keys),
        name="index",
    )(index_key, *pieces)
    other_part = pair_swap(part)

    powers, peaks, lses = pl.pallas_call(
        score_kernel,
        out_shape=(
            shape((local_heads, queries, keys), f32),
            shape((queries, LANES), f32),
            shape((queries, LANES), f32),
        ),
        in_specs=[VMEM_WHOLE] * 4,
        out_specs=(VMEM_WHOLE,) * 3,
        scratch_shapes=[pltpu.VMEM((HEADS_A_STEP * queries, latent_dim), bf16)] * 3,
        compiler_params=params(4 * local_heads * queries * keys),
        name="scores",
    )(rows, w_uk, latent_t, bias)

    send, index_powers, index_peaks = pl.pallas_call(
        functools.partial(stats_kernel, offsets, own_rows, local_heads),
        out_shape=(
            shape((ctx, 1, (packed_rows(local_heads, queries)[1] + 1) * LANES), f32),
            shape((queries, keys), f32),
            shape((queries, LANES), f32),
        ),
        in_specs=[VMEM_WHOLE] * 4,
        out_specs=(VMEM_WHOLE,) * 3,
        compiler_params=params(),
        name="stats",
    )(part, other_part, bias, lses)
    every = lax.all_to_all(send, "ctx", 0, 0, tiled=True)

    target, predicted = pl.pallas_call(
        functools.partial(target_kernel, local_heads),
        out_shape=(shape((queries, keys), f32), shape((queries, keys), f32)),
        in_specs=[VMEM_WHOLE] * 5,
        out_specs=(VMEM_WHOLE,) * 2,
        compiler_params=params(4 * local_heads * queries * keys),
        name="target",
    )(every, peaks, index_peaks, powers, index_powers)
    other_target = pair_swap(target)

    slopes, to_owner = pl.pallas_call(
        functools.partial(slope_kernel, offsets, own_rows, keys * ctx),
        out_shape=(
            shape((index_local * queries, keys), bf16),
            shape((ctx, own_rows, index_local * INDEX_DIM), bf16),
        ),
        in_specs=[VMEM_WHOLE] * 5,
        out_specs=(VMEM_WHOLE,) * 2,
        compiler_params=params(4 * index_local * queries * keys),
        name="slopes",
    )(predicted, target, other_target, gate, index_key)
    grad_query = jnp.sum(lax.all_to_all(to_owner, "ctx", 0, 0, tiled=True).astype(f32), axis=0)

    grad_key_part = lax.dot_general(slopes, stack, (((0,), (0,)), ((), ())), preferred_element_type=f32)
    grad_key = grad_key_part + pair_swap(grad_key_part)
    along = (grad_query * index_query.astype(f32)).reshape(own_rows, index_local, INDEX_DIM)
    grad_weight = jnp.sum(along, axis=2) / head_weight.astype(f32)
    return grad_query, grad_key, grad_weight


def solution(mesh):
    placed = (
        P("ctx", "head"),
        P("head", None, None),
        P(None, "ctx"),
        P("ctx", "head"),
        P("ctx", None),
        P("ctx", "head"),
        P(),
        P(),
    )
    return jax.shard_map(
        shards,
        mesh=mesh,
        in_specs=placed,
        out_specs=(P("ctx", "head"), P("ctx", None), P("ctx", "head")),
        check_vma=False,
    )
```

```python
import functools
import math

import jax
import jax.numpy as jnp
from jax import lax
from jax.experimental import pallas as pl
from jax.experimental.pallas import tpu as pltpu
from jax.sharding import PartitionSpec as P


MLA_HEADS = 128
ROPE_DIM = 64
NOPE_DIM = 128
INDEX_HEADS = 64
INDEX_DIM = 128
WIDTH = NOPE_DIM + ROPE_DIM
LANES = 128


MASKED = -1e30
HEADS_A_STEP = 8
LOG2E = math.log2(math.e)
f32 = jnp.float32
bf16 = jnp.bfloat16
HBM_WHOLE = pl.BlockSpec(memory_space=pltpu.HBM)
VMEM_WHOLE = pl.BlockSpec(memory_space=pltpu.VMEM)
SMEM_WHOLE = pl.BlockSpec(memory_space=pltpu.SMEM)


def exchange_stages(size):
    bits = size.bit_length() - 1
    stages = []
    while bits > 0:
        take = 2 if bits >= 2 else 1
        bits -= take
        stages.append([k << bits for k in range(1 << take)])
    return stages


def send(block, axis, size, mask):
    return lax.ppermute(block, axis, [(i, i ^ mask) for i in range(size)])


def gather_pieces(own, axis, size):
    *stages, last = exchange_stages(size)
    early = [send(own, axis, size, mask) for mask in last[1:]]
    blocks, offsets = own, [0]
    for masks in stages:
        parts = [blocks] + [send(blocks, axis, size, mask) for mask in masks[1:]]
        blocks = jnp.concatenate(parts[(len(offsets) == 1) :], axis=0)
        if len(offsets) == 1:
            blocks = blocks if len(stages) == 1 else jnp.concatenate([own, blocks], axis=0)
        offsets = [mask ^ offset for mask in masks for offset in offsets]
    if not stages:
        return [own, *early], list(last)
    rest = blocks if len(stages) == 1 else blocks[1:]
    late = [send(rest, axis, size, mask) for mask in last[1:]]
    pieces, order = [own, rest], list(offsets)
    for mask, own_piece, rest_piece in zip(last[1:], early, late, strict=True):
        pieces += [own_piece, rest_piece]
        order += [mask ^ offset for offset in offsets]
    return pieces, order


def pair_swap(part):
    return lax.ppermute(part, "head", [(0, 1), (1, 0)])


def params(held=0):
    return pltpu.CompilerParams(vmem_limit_bytes=(16 << 20) if held <= (16 << 20) else (60 << 20))


def row_column(shape, values):
    row = lax.broadcasted_iota(jnp.int32, shape, 0)
    out = jnp.zeros(shape, jnp.int32)
    for i, value in enumerate(values):
        out = jnp.where(row == i, value, out)
    return out


def bias_kernel(offsets, own_rows, keys, pos_ref, start_ref, bias_ref):
    queries = bias_ref.shape[0]
    me = lax.axis_index("ctx")
    places = [(me ^ int(off)) * own_rows + r for off in offsets for r in range(own_rows)]
    ids = me * keys + lax.broadcasted_iota(jnp.int32, (queries, keys), 1)
    first = row_column((queries, LANES), [start_ref[p] for p in places])[:, :1]
    last = row_column((queries, LANES), [pos_ref[p] for p in places])[:, :1]
    bias_ref[...] = jnp.where((ids >= first) & (ids <= last), 0.0, MASKED)


def fetch_kernel(*refs):
    count = (len(refs) - 1) // 2
    copies = [pltpu.make_async_copy(refs[i], refs[count + i], refs[-1].at[i]) for i in range(count)]
    for copy in copies:
        copy.start()
    for copy in copies:
        copy.wait()


def index_kernel(own_rows, heads, query_cols, key_ref, *refs):
    *piece_refs, rows_ref, gate_ref, part_ref, stack_ref = refs
    queries = rows_ref.shape[0]
    keys = key_ref.shape[0]
    at = 0
    for piece in piece_refs:
        for i in range(piece.shape[0]):
            rows_ref[at : at + own_rows, :] = piece[i]
            at += own_rows
    scale = (INDEX_DIM * INDEX_HEADS) ** (-0.5)
    weights = rows_ref[:, query_cols + heads * INDEX_DIM :].astype(f32) * scale
    for j in range(heads):
        col = query_cols + j * INDEX_DIM
        stack_ref[j * queries : (j + 1) * queries, :] = rows_ref[:, col : col + INDEX_DIM]
    chunk = 8
    total = jnp.zeros((queries, keys), f32)
    for c in range(0, heads, chunk):
        left = stack_ref[c * queries : (c + chunk) * queries, :]
        dotted = lax.dot_general(left, key_ref[...], (((1,), (1,)), ((), ())), preferred_element_type=f32)
        for j in range(chunk):
            one = dotted[j * queries : (j + 1) * queries]
            gate = jnp.where(one > 0, weights[:, c + j : c + j + 1], 0.0)
            gate_ref[c + j] = gate
            total = total + gate * one
    part_ref[...] = total


def score_kernel(rows_ref, w_ref, latent_ref, bias_ref, power_ref, peak_ref, lse_ref, *left_refs):
    queries = bias_ref.shape[0]
    heads, _, rank = w_ref.shape
    chunk = HEADS_A_STEP
    scale = WIDTH ** (-0.5)
    lane = lax.broadcasted_iota(jnp.int32, (queries, LANES), 1)

    def absorb(c, left_ref):
        for i in range(chunk):
            h = c * chunk + i
            own = rows_ref[:, h * WIDTH : (h + 1) * WIDTH]
            folded = jnp.dot(own[:, :NOPE_DIM], w_ref[h], preferred_element_type=f32)
            left_ref[i * queries : (i + 1) * queries, :rank] = folded.astype(bf16)
            left_ref[i * queries : (i + 1) * queries, rank:] = own[:, NOPE_DIM:]

    peaks = jnp.zeros((queries, LANES), f32)
    lses = jnp.zeros((queries, LANES), f32)
    absorb(0, left_refs[0])
    for c in range(heads // chunk):
        raw = jnp.dot(left_refs[c % len(left_refs)][...], latent_ref[...], preferred_element_type=f32)
        if c + 1 < heads // chunk:
            absorb(c + 1, left_refs[(c + 1) % len(left_refs)])
        for i in range(chunk):
            h = c * chunk + i
            one = raw[i * queries : (i + 1) * queries] + bias_ref[...]
            top = jnp.max(one, axis=1, keepdims=True)
            power = jnp.exp2((one - top) * (scale * LOG2E))
            power_ref[h] = power
            total = jnp.sum(power, axis=1, keepdims=True)
            peak = top * scale
            peaks = jnp.where(lane == h, peak, peaks)
            lses = jnp.where(lane == h, peak + jnp.log(total), lses)
    peak_ref[...] = peaks
    lse_ref[...] = lses


def packed_rows(heads, queries):
    a_row = LANES // heads
    return a_row, queries // a_row


def stats_kernel(offsets, own_rows, heads, part_ref, other_ref, bias_ref, lse_ref, send_ref, power_ref, peak_ref):
    queries = part_ref.shape[0]
    me = lax.axis_index("ctx")
    score = (part_ref[...] + other_ref[...]) + bias_ref[...]
    peak = jnp.max(score, axis=1, keepdims=True)
    power = jnp.exp(score - peak)
    power_ref[...] = power
    lse = peak + jnp.log(jnp.sum(power, axis=1, keepdims=True))
    lane = lax.broadcasted_iota(jnp.int32, (queries, LANES), 1)
    row = lax.broadcasted_iota(jnp.int32, (queries, LANES), 0)
    stats = jnp.where(lane == heads, lse, lse_ref[...])
    peak_ref[...] = jnp.broadcast_to(peak, (queries, LANES))
    place = {int(off): b for b, off in enumerate(offsets)}
    a_row, count = packed_rows(heads, queries)
    for away in range(len(offsets)):
        order = [place[away ^ int(off)] for off in offsets]
        moved = jnp.concatenate([stats[b * own_rows : (b + 1) * own_rows] for b in order], axis=0)
        packed = moved[:count]
        for i in range(1, a_row):
            packed = jnp.where(lane[:count] < i * heads, packed, pltpu.roll(moved[i * count : (i + 1) * count], i * heads, 1))
        line = jnp.sum(jnp.where(lane == row, moved[:, heads : heads + 1], 0.0), axis=0, keepdims=True)
        for i in range(count):
            send_ref[me ^ away, :, i * LANES : (i + 1) * LANES] = packed[i : i + 1]
        send_ref[me ^ away, :, count * LANES :] = line


def target_kernel(heads, every_ref, peak_ref, index_peak_ref, power_ref, index_power_ref, target_ref, predicted_ref):
    queries = peak_ref.shape[0]
    a_row, count = packed_rows(heads, queries)
    lines = []
    for i in range(count + 1):
        part = every_ref[:, 0, i * LANES : (i + 1) * LANES]
        top = jnp.max(part, axis=0, keepdims=True)
        lines.append(top + jnp.log(jnp.sum(jnp.exp(part - top), axis=0, keepdims=True)))
    packed = jnp.concatenate(lines[:count], axis=0)
    whole = jnp.concatenate([packed] + [pltpu.roll(packed, LANES - i * heads, 1) for i in range(1, a_row)], axis=0)
    lane = lax.broadcasted_iota(jnp.int32, (queries, LANES), 1)
    row = lax.broadcasted_iota(jnp.int32, (queries, LANES), 0)
    index_whole = jnp.sum(jnp.where(lane == row, lines[count], 0.0), axis=1, keepdims=True)
    factor = jnp.exp(peak_ref[...] - whole)
    predicted_ref[...] = index_power_ref[...] * jnp.exp(index_peak_ref[:, :1] - index_whole)
    total = power_ref[0] * factor[:, :1]
    for h in range(1, heads):
        total = total + power_ref[h] * factor[:, h : h + 1]
    target_ref[...] = total


def slope_kernel(offsets, own_rows, all_keys, predicted_ref, target_ref, other_ref, gate_ref, key_ref, slope_ref, send_ref):
    heads, queries, _ = gate_ref.shape
    me = lax.axis_index("ctx")
    target = (target_ref[...] + other_ref[...]) / MLA_HEADS
    misfit = (predicted_ref[...] - target) * all_keys
    chunk = 8
    for c in range(0, heads, chunk):
        slopes = jnp.concatenate([(misfit * gate_ref[c + j]).astype(bf16) for j in range(chunk)], axis=0)
        slope_ref[c * queries : (c + chunk) * queries, :] = slopes
        grad = jnp.dot(slopes, key_ref[...], preferred_element_type=f32).astype(send_ref.dtype)
        for j in range(chunk):
            col = (c + j) * INDEX_DIM
            for b, off in enumerate(offsets):
                at = j * queries + b * own_rows
                send_ref[me ^ int(off), :, col : col + INDEX_DIM] = grad[at : at + own_rows]


def shards(q_heads, w_uk, latent_t, index_query, index_key, head_weight, query_pos, key_start):
    own_rows = q_heads.shape[0]
    ctx = lax.axis_size("ctx")
    latent_dim, keys = latent_t.shape
    local_heads, _, _ = w_uk.shape
    index_local = head_weight.shape[1]
    queries = own_rows * ctx
    shape = jax.ShapeDtypeStruct

    pad = jnp.zeros((own_rows, -index_local % LANES), bf16)
    own = jnp.concatenate([q_heads, index_query, head_weight, pad], axis=1)
    pieces, offsets = gather_pieces(own[None], "ctx", ctx)

    bias = pl.pallas_call(
        functools.partial(bias_kernel, offsets, own_rows, keys),
        out_shape=shape((queries, keys), f32),
        in_specs=[SMEM_WHOLE] * 2,
        out_specs=VMEM_WHOLE,
        compiler_params=params(),
        name="bias",
    )(query_pos, key_start)
    held = (w_uk, latent_t, index_key)
    w_uk, latent_t, index_key = pl.pallas_call(
        fetch_kernel,
        out_shape=tuple(shape(a.shape, a.dtype) for a in held),
        in_specs=[HBM_WHOLE] * len(held),
        out_specs=(VMEM_WHOLE,) * len(held),
        scratch_shapes=[pltpu.SemaphoreType.DMA((len(held),))],
        compiler_params=params(),
        name="fetch",
    )(*held)

    rows, gate, part, stack = pl.pallas_call(
        functools.partial(index_kernel, own_rows, index_local, q_heads.shape[1]),
        out_shape=(
            shape((queries, own.shape[1]), bf16),
            shape((index_local, queries, keys), f32),
            shape((queries, keys), f32),
            shape((index_local * queries, INDEX_DIM), bf16),
        ),
        in_specs=[VMEM_WHOLE] * (1 + len(pieces)),
        out_specs=(VMEM_WHOLE,) * 4,
        compiler_params=params(4 * index_local * queries * keys),
        name="index",
    )(index_key, *pieces)
    other_part = pair_swap(part)

    powers, peaks, lses = pl.pallas_call(
        score_kernel,
        out_shape=(
            shape((local_heads, queries, keys), f32),
            shape((queries, LANES), f32),
            shape((queries, LANES), f32),
        ),
        in_specs=[VMEM_WHOLE] * 4,
        out_specs=(VMEM_WHOLE,) * 3,
        scratch_shapes=[pltpu.VMEM((HEADS_A_STEP * queries, latent_dim), bf16)] * 3,
        compiler_params=params(4 * local_heads * queries * keys),
        name="scores",
    )(rows, w_uk, latent_t, bias)

    send, index_powers, index_peaks = pl.pallas_call(
        functools.partial(stats_kernel, offsets, own_rows, local_heads),
        out_shape=(
            shape((ctx, 1, (packed_rows(local_heads, queries)[1] + 1) * LANES), f32),
            shape((queries, keys), f32),
            shape((queries, LANES), f32),
        ),
        in_specs=[VMEM_WHOLE] * 4,
        out_specs=(VMEM_WHOLE,) * 3,
        compiler_params=params(),
        name="stats",
    )(part, other_part, bias, lses)
    every = lax.all_to_all(send, "ctx", 0, 0, tiled=True)

    target, predicted = pl.pallas_call(
        functools.partial(target_kernel, local_heads),
        out_shape=(shape((queries, keys), f32), shape((queries, keys), f32)),
        in_specs=[VMEM_WHOLE] * 5,
        out_specs=(VMEM_WHOLE,) * 2,
        compiler_params=params(4 * local_heads * queries * keys),
        name="target",
    )(every, peaks, index_peaks, powers, index_powers)
    other_target = pair_swap(target)

    slopes, to_owner = pl.pallas_call(
        functools.partial(slope_kernel, offsets, own_rows, keys * ctx),
        out_shape=(
            shape((index_local * queries, keys), bf16),
            shape((ctx, own_rows, index_local * INDEX_DIM), bf16),
        ),
        in_specs=[VMEM_WHOLE] * 5,
        out_specs=(VMEM_WHOLE,) * 2,
        compiler_params=params(4 * index_local * queries * keys),
        name="slopes",
    )(predicted, target, other_target, gate, index_key)
    from_all = lax.all_to_all(to_owner, "ctx", 0, 0, tiled=True)
    grad_query = jnp.sum(from_all.astype(f32), axis=0)

    grad_key_part = lax.dot_general(slopes, stack, (((0,), (0,)), ((), ())), preferred_element_type=f32)
    other_key = pair_swap(grad_key_part)
    grad_key = grad_key_part + other_key
    along = (grad_query * index_query.astype(f32)).reshape(own_rows, index_local, INDEX_DIM)
    grad_weight = jnp.sum(along, axis=2) / head_weight.astype(f32)
    return grad_query, grad_key, grad_weight


def solution(mesh):
    placed = (
        P("ctx", "head"),
        P("head", None, None),
        P(None, "ctx"),
        P("ctx", "head"),
        P("ctx", None),
        P("ctx", "head"),
        P(),
        P(),
    )
    return jax.shard_map(
        shards,
        mesh=mesh,
        in_specs=placed,
        out_specs=(P("ctx", "head"), P("ctx", None), P("ctx", "head")),
        check_vma=False,
    )
```
